128 devices in a mesh: lon: 16 (over y_hi, z, core), mem: 8 (over x, y_lo).
Axes of the slice: x: 4, y: 4 (y_hi: 2, y_lo: 2; y = y_hi * 2 + y_lo), z: 4, core: 2. Of those that a mesh axis runs over, the one named last changes fastest.
Arguments:
- alpha: bfloat16 [80, 128, 512, 128], P('mem', 'lon'), may hold values from -6 to 6
- ens_pert: bfloat16 [80, 128, 512, 128], P('mem', None, 'lon'), may hold values from -6 to 6
- vert_sqrt: bfloat16 [128, 128], replicated, may hold values from -0.5 to 0.5
- lat_sqrt: bfloat16 [128, 128], replicated, may hold values from -0.5 to 0.5
Outputs:
- increment: float32 [128, 512, 128], P('mem', 'lon')
The draws below stay inside these ranges and needn't reach their ends.
All inputs are finite; a program needn't handle non-finite values.
Results may differ from the reference program's by a relative error of at most 0.0042.
Values may be sent and summed in bfloat16 or wider, within the bound.
A program may use at most 128 MiB of HBM per device.

```python
import math
import jax
import jax.numpy as jnp
from jax import lax

LEV = 128
LAT = 128
MEMBERS = 80
LON = 512


def block_scale(own_key, dims, pieces, low, high):
    gain = 1.0
    for dim, blocks in pieces:
        draws = jax.random.uniform(jax.random.fold_in(jax.random.fold_in(own_key, 6), dim), (blocks,), jnp.float32, low / len(pieces), high / len(pieces))
        gain = gain * jnp.repeat(jnp.exp(draws), dims[dim] // blocks).reshape((-1,) + (1,) * (len(dims) - 1 - dim))
    return gain


def bell_draw(stream_key, shape, deviation, limit, cuts=(), kind=jnp.bfloat16):
    gain = block_scale(stream_key, shape, cuts, -0.22, 0.18) if cuts else 1.0
    entries = jax.random.normal(stream_key, shape, jnp.float32) * deviation * gain
    return jnp.minimum(jnp.maximum(entries, -limit), limit).astype(kind)


def setup_inputs(seed: int = 0) -> dict:
    seeds = jax.random.split(jax.random.key(seed), 5)
    alpha = bell_draw(seeds[0], (MEMBERS, LEV, LON, LAT), 1.0, 6.0, ((0, 8), (1, 16)))
    ens_pert = bell_draw(seeds[1], (MEMBERS, LEV, LON, LAT), 1.0, 6.0, ((0, 8), (2, 16)))
    vert_sqrt = bell_draw(seeds[2], (LEV, LEV), LEV ** -0.5, 0.5)
    lat_sqrt = bell_draw(seeds[3], (LAT, LAT), LAT ** -0.5, 0.5)
    return {"alpha": alpha, "ens_pert": ens_pert, "vert_sqrt": vert_sqrt, "lat_sqrt": lat_sqrt}


def reference(alpha, ens_pert, vert_sqrt, lat_sqrt):
    factor = 1.0 / math.sqrt(MEMBERS)
    vert_full = vert_sqrt.astype(jnp.float32)
    lat_full = lat_sqrt.astype(jnp.float32)

    def member_step(total, pair):
        member_alpha, member_pert = pair
        vertical = jnp.einsum('kl,lxi->kxi', vert_full, member_alpha.astype(jnp.float32), precision=lax.Precision.HIGHEST).astype(jnp.bfloat16)
        localized = jnp.einsum('kxi,ij->kxj', vertical.astype(jnp.float32), lat_full, precision=lax.Precision.HIGHEST)
        return (total + member_pert.astype(jnp.float32) * localized, None)
    initial = jnp.zeros((LEV, LON, LAT), jnp.float32)
    total, unused = lax.scan(member_step, initial, (alpha, ens_pert))
    return total * factor
```

```python
import functools
import math

import jax
import jax.numpy as jnp
from jax import lax
from jax.experimental import pallas as pl
from jax.experimental.pallas import tpu as pltpu
from jax.sharding import PartitionSpec as P

MESH = pl.DeviceIdType.MESH
ROWS = 8
PAIR = 2
WINDOW = 20


def kernel(
    factor, n_lon, n_mem, alpha_ref, pert_ref, vert_ref, lat_ref, out_ref,
    columns, perts, kron, lat_two, total, parts, arrived,
    own_sem, pert_sem, send_sem, recv_sem, part_send_sem, part_recv_sem,
):
    lon, mem = lax.axis_index("lon"), lax.axis_index("mem")
    members, levels_own = alpha_ref.shape[0], alpha_ref.shape[1]
    levels = levels_own * n_lon
    own_rows = pert_ref.shape[2]
    width = lat_ref.shape[0]
    chunks, pairs = own_rows // ROWS, members // PAIR
    units = chunks * pairs
    stacked = levels * ROWS
    levels_out = levels // n_mem

    def lon_peer(dy, dz, dc):
        y, z, c = lon // 8, (lon // 2) % 4, lon % 2
        return ((y + dy) % 2) * 8 + ((z + dz) % 4) * 2 + (c + dc) % 2

    lon_peers = [
        lon_peer(dy, dz, dc)
        for dz in (2, 1, 3, 0) for dy in (1, 0) for dc in (0, 1)
        if (dy, dz, dc) != (0, 0, 0)
    ]
    mem_peers = [(mem + step) % n_mem for step in range(1, n_mem)]

    barrier = pltpu.get_barrier_semaphore()
    for peer in lon_peers:
        pl.semaphore_signal(barrier, inc=1, device_id={"lon": peer, "mem": mem}, device_id_type=MESH)
    for peer in mem_peers:
        pl.semaphore_signal(barrier, inc=1, device_id={"lon": lon, "mem": peer}, device_id_type=MESH)

    def own_copy(chunk):
        rows = pl.ds(pl.multiple_of(lon * own_rows + chunk * ROWS, ROWS), ROWS)
        return pltpu.make_async_copy(
            alpha_ref.at[:, :, rows, :],
            columns.at[chunk, :, pl.ds(lon * levels_own, levels_own)],
            own_sem.at[chunk],
        )

    def pert_copy(chunk):
        rows = pl.ds(pl.multiple_of(chunk * ROWS, ROWS), ROWS)
        return pltpu.make_async_copy(pert_ref.at[:, :, rows, :], perts.at[chunk], pert_sem.at[chunk])

    def send(unit):
        chunk, pair = unit // pairs, unit % pairs
        group = pl.ds(pair * PAIR, PAIR)
        for peer in lon_peers:
            rows = pl.ds(pl.multiple_of(peer * own_rows + chunk * ROWS, ROWS), ROWS)
            pltpu.make_async_remote_copy(
                src_ref=alpha_ref.at[group, :, rows, :],
                dst_ref=columns.at[chunk, group, pl.ds(lon * levels_own, levels_own)],
                send_sem=send_sem, recv_sem=recv_sem.at[unit],
                device_id={"lon": peer, "mem": mem}, device_id_type=MESH,
            ).start()

    pl.semaphore_wait(barrier, len(lon_peers) + len(mem_peers))

    def first_sends(unit, carry):
        send(unit)
        return carry

    lax.fori_loop(0, min(WINDOW, units), first_sends, 0)
    for chunk in range(chunks):
        own_copy(chunk).start()
        pert_copy(chunk).start()

    wide = (levels, stacked)
    spread = (
        lax.broadcasted_iota(jnp.int32, wide, 1) // ROWS == lax.broadcasted_iota(jnp.int32, wide, 0)
    ).astype(jnp.bfloat16)
    band = (
        lax.broadcasted_iota(jnp.int32, (levels, levels // ROWS), 0) // ROWS
        == lax.broadcasted_iota(jnp.int32, (levels, levels // ROWS), 1)
    ).astype(jnp.bfloat16)

    same = lax.broadcasted_iota(jnp.int32, wide, 0) % ROWS == lax.broadcasted_iota(jnp.int32, wide, 1) % ROWS

    def build(block, carry):
        tall = levels // ROWS
        some = vert_ref[pl.ds(pl.multiple_of(block * tall, tall), tall), :]
        tallest = jnp.dot(band, some, preferred_element_type=jnp.float32).astype(jnp.bfloat16)
        full = jnp.dot(tallest, spread, preferred_element_type=jnp.float32)
        kron[pl.ds(pl.multiple_of(block * levels, levels), levels), :] = jnp.where(same, full, 0.0).astype(jnp.bfloat16)
        return carry

    lax.fori_loop(0, stacked // levels, build, 0)
    lat_two[...] = jnp.zeros_like(lat_two)
    lat_two[pl.ds(0, width), pl.ds(0, width)] = lat_ref[...]
    lat_two[pl.ds(width, width), pl.ds(width, width)] = lat_ref[...]

    def part_copy(chunk, peer):
        return pltpu.make_async_remote_copy(
            src_ref=parts.at[chunk, pl.ds(peer * levels_out, levels_out)],
            dst_ref=arrived.at[chunk, mem],
            send_sem=part_send_sem, recv_sem=part_recv_sem.at[chunk],
            device_id={"lon": lon, "mem": peer}, device_id_type=MESH,
        )

    def finish(chunk):
        others = arrived.at[chunk, pl.ds(0, n_mem - 1)]
        pltpu.make_async_copy(others, others, part_recv_sem.at[chunk]).wait()
        value = arrived[chunk, 0].astype(jnp.float32)
        for source in range(1, n_mem):
            value = value + arrived[chunk, source].astype(jnp.float32)
        out_ref[:, pl.ds(pl.multiple_of(chunk * ROWS, ROWS), ROWS), :] = value

    def chunk_step(chunk, carry):
        own_copy(chunk).wait()
        pert_copy(chunk).wait()
        total[...] = jnp.zeros_like(total)

        def unit_step(pair, carry):
            unit = chunk * pairs + pair
            if WINDOW < units:
                @pl.when(unit + WINDOW < units)
                def _():
                    send(unit + WINDOW)
            landed = columns.at[chunk, pl.ds(pair * PAIR, PAIR), pl.ds(0, levels - levels_own)]
            pltpu.make_async_copy(landed, landed, recv_sem.at[unit]).wait()
            both = jnp.concatenate(
                [columns[chunk, pair * PAIR + k].reshape(stacked, width) for k in range(PAIR)], axis=1
            )
            vertical = jnp.dot(kron[...], both, preferred_element_type=jnp.float32).astype(jnp.bfloat16)
            localized = jnp.dot(vertical, lat_two[...], preferred_element_type=jnp.float32)
            value = total[...]
            for k in range(PAIR):
                pert = perts[chunk, pair * PAIR + k].reshape(stacked, width).astype(jnp.float32)
                value = value + pert * localized[:, k * width : (k + 1) * width]
            total[...] = value
            return carry

        lax.fori_loop(0, pairs, unit_step, 0)
        parts[chunk] = (total[...] * factor).astype(jnp.bfloat16).reshape(levels, ROWS, width)
        for peer in mem_peers:
            part_copy(chunk, peer).start()
        arrived[chunk, mem] = parts[chunk, pl.ds(mem * levels_out, levels_out)]

        @pl.when(chunk > 0)
        def _():
            finish(chunk - 1)

        return carry

    lax.fori_loop(0, chunks, chunk_step, 0)
    finish(chunks - 1)

    sent = columns.at[:, :, pl.ds(0, levels - levels_own)]
    pltpu.make_async_copy(sent, sent, send_sem).wait()
    sent = arrived.at[:, pl.ds(0, n_mem - 1)]
    pltpu.make_async_copy(sent, sent, part_send_sem).wait()


def local(alpha, ens_pert, vert_sqrt, lat_sqrt):
    n_lon, n_mem = lax.axis_size("lon"), lax.axis_size("mem")
    members, levels_own, _, width = alpha.shape
    _, levels, own_rows, _ = ens_pert.shape
    chunks = own_rows // ROWS
    units = chunks * (members // PAIR)
    stacked = levels * ROWS
    levels_out = levels // n_mem
    factor = 1.0 / math.sqrt(members * n_mem)
    vmem = pl.BlockSpec(memory_space=pltpu.VMEM)
    hbm = pl.BlockSpec(memory_space=pl.ANY)
    return pl.pallas_call(
        functools.partial(kernel, factor, n_lon, n_mem),
        out_shape=jax.ShapeDtypeStruct((levels_out, own_rows, width), jnp.float32),
        in_specs=[hbm, hbm, vmem, vmem],
        out_specs=vmem,
        scratch_shapes=[
            pltpu.VMEM((chunks, members, levels, ROWS, width), jnp.bfloat16),
            pltpu.VMEM((chunks, members, levels, ROWS, width), jnp.bfloat16),
            pltpu.VMEM((stacked, stacked), jnp.bfloat16),
            pltpu.VMEM((PAIR * width, PAIR * width), jnp.bfloat16),
            pltpu.VMEM((stacked, width), jnp.float32),
            pltpu.VMEM((chunks, levels, ROWS, width), jnp.bfloat16),
            pltpu.VMEM((chunks, n_mem, levels_out, ROWS, width), jnp.bfloat16),
            pltpu.SemaphoreType.DMA((chunks,)),
            pltpu.SemaphoreType.DMA((chunks,)),
            pltpu.SemaphoreType.DMA,
            pltpu.SemaphoreType.DMA((units,)),
            pltpu.SemaphoreType.DMA,
            pltpu.SemaphoreType.DMA((chunks,)),
        ],
        compiler_params=pltpu.CompilerParams(
            collective_id=0, has_side_effects=True, vmem_limit_bytes=60 * 2**20
        ),
    )(alpha, ens_pert, vert_sqrt, lat_sqrt)


def solution(mesh):
    placed = (P("mem", "lon", None, None), P("mem", None, "lon", None), P(), P())
    return jax.shard_map(
        local, mesh=mesh, in_specs=placed, out_specs=P("mem", "lon", None), check_vma=False
    )
```

```python
import functools
import math

import jax
import jax.numpy as jnp
from jax import lax
from jax.experimental import pallas as pl
from jax.experimental.pallas import tpu as pltpu
from jax.sharding import PartitionSpec as P

MESH = pl.DeviceIdType.MESH
ROWS = 8
PAIR = 2
WINDOW = 15
LIMIT = 54
HALF = True
STAGGER = True


def kernel(
    factor, n_lon, n_mem, alpha_ref, pert_ref, vert_ref, lat_ref, out_ref,
    columns, perts, staged, vert, kron, lat_two, total, parts, runs, held, halves, second, arrived,
    stage_sem, small_sem, own_sem, pert_sem, send_sem, recv_sem,
    run_send, run_recv, half_send, half_recv, last_send, last_recv,
):
    lon, mem = lax.axis_index("lon"), lax.axis_index("mem")
    members, levels_own = alpha_ref.shape[0], alpha_ref.shape[1]
    levels = levels_own * n_lon
    own_rows = pert_ref.shape[2]
    width = lat_ref.shape[0]
    chunks, pairs = own_rows // ROWS, members // PAIR
    units = chunks * pairs
    stacked = levels * ROWS
    levels_out = levels // n_mem
    n_run = n_mem // 2
    mem_x, mem_y = mem // 2, mem % 2
    last = chunks - 1

    def lon_peer(dy, dz, dc):
        y, z, c = lon // 8, (lon // 2) % 4, lon % 2
        return ((y + dy) % 2) * 8 + ((z + dz) % 4) * 2 + (c + dc) % 2

    lon_peers = [
        lon_peer(dy, dz, dc)
        for dz in (2, 1, 3, 0) for dy in (1, 0) for dc in (0, 1)
        if (dy, dz, dc) != (0, 0, 0)
    ]
    mem_peers = [(mem + step) % n_mem for step in range(1, n_mem)]

    def wait_for(ref, sem):
        pltpu.make_async_copy(ref, ref, sem).wait()

    barrier = pltpu.get_barrier_semaphore()
    for peer in lon_peers:
        pl.semaphore_signal(barrier, inc=1, device_id={"lon": peer, "mem": mem}, device_id_type=MESH)
    for peer in mem_peers:
        pl.semaphore_signal(barrier, inc=1, device_id={"lon": lon, "mem": peer}, device_id_type=MESH)

    def own_copy(chunk):
        rows = pl.ds(pl.multiple_of(lon * own_rows + chunk * ROWS, ROWS), ROWS)
        return pltpu.make_async_copy(
            alpha_ref.at[:, :, rows, :],
            columns.at[chunk, :, pl.ds(lon * levels_own, levels_own)],
            own_sem.at[chunk],
        )

    def pert_copy(chunk):
        rows = pl.ds(pl.multiple_of(chunk * ROWS, ROWS), ROWS)
        return pltpu.make_async_copy(pert_ref.at[:, :, rows, :], perts.at[chunk], pert_sem.at[chunk])

    def send_to(peer, source, unit):
        chunk, pair = unit // pairs, unit % pairs
        group = pl.ds(pair * PAIR, PAIR)
        rows = pl.ds(pl.multiple_of(peer * own_rows + chunk * ROWS, ROWS), ROWS)
        pltpu.make_async_remote_copy(
            src_ref=source.at[group, :, rows, :],
            dst_ref=columns.at[chunk, group, pl.ds(lon * levels_own, levels_own)],
            send_sem=send_sem, recv_sem=recv_sem.at[unit],
            device_id={"lon": peer, "mem": mem}, device_id_type=MESH,
        ).start()

    def send(unit, carry):
        for peer in lon_peers:
            send_to(peer, alpha_ref, unit)
        return carry

    def send_late(step):
        core, pair = step // pairs, step % pairs
        unit = last * pairs + pair
        for dz in (2, 1, 3, 0):
            for dy in (1, 0):
                if (dy, dz) != (0, 0):
                    send_to(lon_peer(dy, dz, core + lon), alpha_ref, unit)

        @pl.when(lon % 2 != core)
        def _():
            send_to(lon_peer(0, 0, 1), alpha_ref, unit)

    def send_ahead(unit):
        early = last * pairs
        if not STAGGER:
            @pl.when(unit < units)
            def _():
                send(unit, 0)
            return

        @pl.when(unit < early)
        def _():
            send(unit, 0)

        @pl.when((unit >= early) & (unit < units))
        def _():
            for step in range(2):
                send_late((unit - early) * 2 + step)

    stage = pltpu.make_async_copy(alpha_ref.at[pl.ds(0, PAIR)], staged, stage_sem)
    stage.start()
    vert_copy = pltpu.make_async_copy(vert_ref, vert, small_sem.at[0])
    vert_copy.start()
    lat_two[...] = jnp.zeros_like(lat_two)
    stage.wait()
    pl.semaphore_wait(barrier, len(lon_peers) + len(mem_peers))

    for peer in lon_peers:
        send_to(peer, staged, 0)
    lax.fori_loop(1, min(WINDOW, units), send, 0)
    lat_copies = [
        pltpu.make_async_copy(
            lat_ref, lat_two.at[pl.ds(k * width, width), pl.ds(k * width, width)], small_sem.at[1 + k]
        )
        for k in range(PAIR)
    ]
    for copy in lat_copies:
        copy.start()
    for chunk in range(chunks):
        own_copy(chunk).start()
        pert_copy(chunk).start()

    wide = (levels, stacked)
    spread = (
        lax.broadcasted_iota(jnp.int32, wide, 1) // ROWS == lax.broadcasted_iota(jnp.int32, wide, 0)
    ).astype(jnp.bfloat16)
    tall = levels // ROWS
    band = (
        lax.broadcasted_iota(jnp.int32, (levels, tall), 0) // ROWS == lax.broadcasted_iota(jnp.int32, (levels, tall), 1)
    ).astype(jnp.bfloat16)
    same = lax.broadcasted_iota(jnp.int32, wide, 0) % ROWS == lax.broadcasted_iota(jnp.int32, wide, 1) % ROWS

    def build(block, carry):
        some = vert[pl.ds(pl.multiple_of(block * tall, tall), tall), :]
        repeated = jnp.dot(band, some, preferred_element_type=jnp.float32).astype(jnp.bfloat16)
        full = jnp.dot(repeated, spread, preferred_element_type=jnp.float32)
        kron[pl.ds(pl.multiple_of(block * levels, levels), levels), :] = jnp.where(same, full, 0.0).astype(jnp.bfloat16)
        return carry

    vert_copy.wait()
    lax.fori_loop(0, stacked // levels, build, 0)
    for copy in lat_copies:
        copy.wait()

    def to_device(src, dst, send_sem, recv_sem, peer):
        pltpu.make_async_remote_copy(
            src_ref=src, dst_ref=dst, send_sem=send_sem, recv_sem=recv_sem,
            device_id={"lon": lon, "mem": peer}, device_id_type=MESH,
        ).start()

    def start_runs(chunk):
        parts[chunk] = (total[...] * factor).astype(jnp.bfloat16).reshape(levels, ROWS, width)
        for step in (2, 1, 3):
            peer = (mem_x + step) % n_run
            to_device(
                parts.at[chunk, pl.ds(peer * 2 * levels_out, 2 * levels_out)],
                runs.at[chunk, mem_x], run_send, run_recv.at[chunk], peer * 2 + mem_y,
            )

    def start_half(chunk):
        wait_for(runs.at[chunk, pl.ds(0, n_run - 1)], run_recv.at[chunk])

        def summed(half):
            first = half * levels_out
            value = parts[chunk, pl.ds(mem_x * 2 * levels_out + first, levels_out)].astype(jnp.float32)
            for step in range(1, n_run):
                source = (mem_x + step) % n_run
                value = value + runs[chunk, source, pl.ds(first, levels_out)].astype(jnp.float32)
            return value

        halves[chunk] = summed(1 - mem_y).astype(jnp.bfloat16)
        held[chunk] = summed(mem_y)
        if HALF:
            to_device(halves.at[chunk], second.at[chunk], half_send, half_recv.at[chunk], mem_x * 2 + 1 - mem_y)

    def finish(chunk):
        if HALF:
            wait_for(second.at[chunk], half_recv.at[chunk])
        out_ref[:, pl.ds(chunk * ROWS, ROWS), :] = held[chunk] + second[chunk].astype(jnp.float32)

    def start_last(peer):
        to_device(
            parts.at[last, pl.ds(peer * levels_out, levels_out)], arrived.at[mem], last_send, last_recv, peer
        )

    def finish_last():
        wait_for(arrived.at[pl.ds(0, n_mem - 1)], last_recv)
        value = parts[last, pl.ds(mem * levels_out, levels_out)].astype(jnp.float32)
        for source in mem_peers:
            value = value + arrived[source].astype(jnp.float32)
        out_ref[:, pl.ds(last * ROWS, ROWS), :] = value

    def landed(chunk, pair):
        wait_for(
            columns.at[chunk, pl.ds(pair * PAIR, PAIR), pl.ds(0, levels - levels_own)],
            recv_sem.at[chunk * pairs + pair],
        )
        return jnp.concatenate(
            [columns[chunk, pair * PAIR + k].reshape(stacked, width) for k in range(PAIR)], axis=1
        )

    def added(value, chunk, pair, both, first_level, n_levels):
        rows = pl.ds(first_level * ROWS, n_levels * ROWS)
        vertical = jnp.dot(kron[rows, :], both, preferred_element_type=jnp.float32).astype(jnp.bfloat16)
        localized = jnp.dot(vertical, lat_two[...], preferred_element_type=jnp.float32)
        for k in range(PAIR):
            pert = perts[chunk, pair * PAIR + k, pl.ds(first_level, n_levels)]
            pert = pert.reshape(n_levels * ROWS, width).astype(jnp.float32)
            value = value + pert * localized[:, k * width : (k + 1) * width]
        return value

    def units_of(chunk, n_pairs):
        own_copy(chunk).wait()
        pert_copy(chunk).wait()
        total[...] = jnp.zeros_like(total)

        def unit_step(pair, carry):
            unit = chunk * pairs + pair

            send_ahead(unit + WINDOW)

            both = landed(chunk, pair)

            @pl.when((chunk > 0) & (pair == jnp.where(chunk < last, 1, 1 - lon % 2)))
            def _():
                start_half(chunk - 1)

            total[...] = added(total[...], chunk, pair, both, 0, levels)
            return carry

        lax.fori_loop(0, n_pairs, unit_step, 0)

    def chunk_step(chunk, carry):
        units_of(chunk, pairs)
        start_runs(chunk)
        return carry

    lax.fori_loop(0, last, chunk_step, 0)
    units_of(last, pairs)
    parts[last] = (total[...] * factor).astype(jnp.bfloat16).reshape(levels, ROWS, width)
    for step in (2, 1, 3, 0):
        run = (mem_x + step) % n_run
        start_last(run * 2 + 1 - mem_y)
        if step:
            start_last(run * 2 + mem_y)
    for chunk in range(last):
        finish(chunk)
    finish_last()

    wait_for(columns.at[:, :, pl.ds(0, levels - levels_own)], send_sem)
    wait_for(runs.at[:, pl.ds(0, n_run - 1)], run_send)
    if HALF:
        wait_for(halves, half_send)
    wait_for(arrived.at[pl.ds(0, n_mem - 1)], last_send)


def local(alpha, ens_pert, vert_sqrt, lat_sqrt):
    n_lon, n_mem = lax.axis_size("lon"), lax.axis_size("mem")
    members, levels_own, _, width = alpha.shape
    _, levels, own_rows, _ = ens_pert.shape
    chunks = own_rows // ROWS
    units = chunks * (members // PAIR)
    stacked = levels * ROWS
    levels_out = levels // n_mem
    factor = 1.0 / math.sqrt(members * n_mem)
    hbm = pl.BlockSpec(memory_space=pltpu.HBM)
    half, full = jnp.bfloat16, jnp.float32
    early = chunks - 1
    return pl.pallas_call(
        functools.partial(kernel, factor, n_lon, n_mem),
        out_shape=pltpu.VMEM((levels_out, own_rows, width), full),
        in_specs=[hbm] * 4,
        out_specs=pl.BlockSpec(memory_space=pltpu.VMEM),
        scratch_shapes=[
            pltpu.VMEM((chunks, members, levels, ROWS, width), half),
            pltpu.VMEM((chunks, members, levels, ROWS, width), half),
            pltpu.VMEM((PAIR, *alpha.shape[1:]), half),
            pltpu.VMEM((levels, levels), half),
            pltpu.VMEM((stacked, stacked), half),
            pltpu.VMEM((PAIR * width, PAIR * width), half),
            pltpu.VMEM((stacked, width), full),
            pltpu.VMEM((chunks, levels, ROWS, width), half),
            pltpu.VMEM((early, n_mem // 2, 2 * levels_out, ROWS, width), half),
            pltpu.VMEM((early, levels_out, ROWS, width), full),
            pltpu.VMEM((early, levels_out, ROWS, width), half),
            pltpu.VMEM((early, levels_out, ROWS, width), half),
            pltpu.VMEM((n_mem, levels_out, ROWS, width), half),
            pltpu.SemaphoreType.DMA,
            pltpu.SemaphoreType.DMA((1 + PAIR,)),
            pltpu.SemaphoreType.DMA((chunks,)),
            pltpu.SemaphoreType.DMA((chunks,)),
            pltpu.SemaphoreType.DMA,
            pltpu.SemaphoreType.DMA((units,)),
            pltpu.SemaphoreType.DMA,
            pltpu.SemaphoreType.DMA((early,)),
            pltpu.SemaphoreType.DMA,
            pltpu.SemaphoreType.DMA((early,)),
            pltpu.SemaphoreType.DMA,
            pltpu.SemaphoreType.DMA,
        ],
        compiler_params=pltpu.CompilerParams(
            collective_id=0, has_side_effects=True, vmem_limit_bytes=LIMIT * 2**20
        ),
    )(*(pltpu.with_memory_space_constraint(x, pltpu.HBM) for x in (alpha, ens_pert, vert_sqrt, lat_sqrt)))


def solution(mesh):
    placed = (P("mem", "lon", None, None), P("mem", None, "lon", None), P(), P())
    return jax.shard_map(
        local, mesh=mesh, in_specs=placed, out_specs=P("mem", "lon", None), check_vma=False
    )
```

```python
import functools
import math

import jax
import jax.numpy as jnp
from jax import lax
from jax.experimental import pallas as pl
from jax.experimental.pallas import tpu as pltpu
from jax.sharding import PartitionSpec as P

MESH = pl.DeviceIdType.MESH
ROWS = 8
PAIR = 2
SEQ = 0
SPLIT = 1
ORDER = 4
LIMIT = 54


def kernel(
    factor, n_lon, n_mem, alpha_ref, pert_ref, vert_ref, lat_ref, out_ref,
    columns, perts, staged, vert, kron, lat_two, total, parts, runs, held, halves, second, arrived,
    stage_sem, small_sem, own_sem, pert_sem, send_sem, recv_sem,
    run_send, run_recv, half_send, half_recv, last_send, last_recv,
):
    lon, mem = lax.axis_index("lon"), lax.axis_index("mem")
    members, levels_own = alpha_ref.shape[0], alpha_ref.shape[1]
    levels = levels_own * n_lon
    own_rows = pert_ref.shape[2]
    width = lat_ref.shape[0]
    chunks, pairs = own_rows // ROWS, members // PAIR
    units = chunks * pairs
    stacked = levels * ROWS
    levels_out = levels // n_mem
    n_run = n_mem // 2
    mem_x, mem_y = mem // 2, mem % 2
    last = chunks - 1

    def lon_peer(dy, dz, dc):
        y, z, c = lon // 8, (lon // 2) % 4, lon % 2
        return ((y + dy) % 2) * 8 + ((z + dz) % 4) * 2 + (c + dc) % 2

    offsets = {
        1: [(dy, dz) for dz in (2, 1, 3, 0) for dy in (1, 0)],
        2: [(1, 2), (0, 1), (0, 3), (1, 0), (0, 2), (1, 1), (1, 3), (0, 0)],
        3: [(0, 0), (1, 0), (0, 1), (0, 3), (1, 1), (1, 3), (0, 2), (1, 2)],
        4: [(1, 2), (1, 1), (1, 3), (1, 0), (0, 2), (0, 1), (0, 3), (0, 0)],
        5: [(0, 2), (0, 1), (0, 3), (1, 2), (1, 1), (1, 3), (1, 0), (0, 0)],
    }[ORDER]
    lon_peers = [
        lon_peer(dy, dz, dc) for dy, dz in offsets for dc in (0, 1) if (dy, dz, dc) != (0, 0, 0)
    ]
    mem_peers = [(mem + step) % n_mem for step in range(1, n_mem)]

    def wait_for(ref, sem):
        pltpu.make_async_copy(ref, ref, sem).wait()

    barrier = pltpu.get_barrier_semaphore()
    for peer in lon_peers:
        pl.semaphore_signal(barrier, inc=1, device_id={"lon": peer, "mem": mem}, device_id_type=MESH)
    for peer in mem_peers:
        pl.semaphore_signal(barrier, inc=1, device_id={"lon": lon, "mem": peer}, device_id_type=MESH)

    def own_copy(chunk):
        rows = pl.ds(pl.multiple_of(lon * own_rows + chunk * ROWS, ROWS), ROWS)
        return pltpu.make_async_copy(
            alpha_ref.at[:, :, rows, :],
            columns.at[chunk, :, pl.ds(lon * levels_own, levels_own)],
            own_sem.at[chunk],
        )

    def pert_copy(chunk):
        rows = pl.ds(pl.multiple_of(chunk * ROWS, ROWS), ROWS)
        return pltpu.make_async_copy(pert_ref.at[:, :, rows, :], perts.at[chunk], pert_sem.at[chunk])

    def send_to(peer, source, unit):
        chunk, pair = unit // pairs, unit % pairs
        rows = pl.ds(pl.multiple_of(peer * own_rows + chunk * ROWS, ROWS), ROWS)
        for k in range(SPLIT):
            group = pl.ds(pair * PAIR + k * (PAIR // SPLIT), PAIR // SPLIT)
            pltpu.make_async_remote_copy(
                src_ref=source.at[group, :, rows, :],
                dst_ref=columns.at[chunk, group, pl.ds(lon * levels_own, levels_own)],
                send_sem=send_sem, recv_sem=recv_sem.at[unit],
                device_id={"lon": peer, "mem": mem}, device_id_type=MESH,
            ).start()

    def send(unit, carry):
        for peer in lon_peers:
            send_to(peer, alpha_ref, unit)
        return carry

    def send_late(core, pair):
        unit = last * pairs + pair
        for dy, dz in offsets:
            if (dy, dz) != (0, 0):
                send_to(lon_peer(dy, dz, core + lon), alpha_ref, unit)

        @pl.when(lon % 2 != core)
        def _():
            send_to(lon_peer(0, 0, 1), alpha_ref, unit)

    stage = pltpu.make_async_copy(alpha_ref.at[pl.ds(0, PAIR)], staged, stage_sem)
    stage.start()
    vert_copy = pltpu.make_async_copy(vert_ref, vert, small_sem.at[0])
    vert_copy.start()
    lat_two[...] = jnp.zeros_like(lat_two)
    stage.wait()
    pl.semaphore_wait(barrier, len(lon_peers) + len(mem_peers))

    for peer in lon_peers:
        send_to(peer, staged, 0)
    lax.fori_loop(1, last * pairs, send, 0)
    orders = [
        [(core, pair) for core in range(2) for pair in range(pairs)],
        [(0, 0), (1, 0), (0, 1), (1, 1), (0, 2), (0, 3), (0, 4), (1, 2), (1, 3), (1, 4)],
        [(0, 0), (1, 0), (0, 1), (0, 2), (0, 3), (0, 4), (1, 1), (1, 2), (1, 3), (1, 4)],
    ]
    for core, pair in orders[SEQ]:
        send_late(core, pair)
    lat_copies = [
        pltpu.make_async_copy(
            lat_ref, lat_two.at[pl.ds(k * width, width), pl.ds(k * width, width)], small_sem.at[1 + k]
        )
        for k in range(PAIR)
    ]
    for copy in lat_copies:
        copy.start()
    for chunk in range(chunks):
        own_copy(chunk).start()
        pert_copy(chunk).start()

    wide = (levels, stacked)
    spread = (
        lax.broadcasted_iota(jnp.int32, wide, 1) // ROWS == lax.broadcasted_iota(jnp.int32, wide, 0)
    ).astype(jnp.bfloat16)
    tall = levels // ROWS
    band = (
        lax.broadcasted_iota(jnp.int32, (levels, tall), 0) // ROWS == lax.broadcasted_iota(jnp.int32, (levels, tall), 1)
    ).astype(jnp.bfloat16)
    same = lax.broadcasted_iota(jnp.int32, wide, 0) % ROWS == lax.broadcasted_iota(jnp.int32, wide, 1) % ROWS

    def build(block, carry):
        some = vert[pl.ds(pl.multiple_of(block * tall, tall), tall), :]
        repeated = jnp.dot(band, some, preferred_element_type=jnp.float32).astype(jnp.bfloat16)
        full = jnp.dot(repeated, spread, preferred_element_type=jnp.float32)
        kron[pl.ds(pl.multiple_of(block * levels, levels), levels), :] = jnp.where(same, full, 0.0).astype(jnp.bfloat16)
        return carry

    vert_copy.wait()
    lax.fori_loop(0, stacked // levels, build, 0)
    for copy in lat_copies:
        copy.wait()

    def to_device(src, dst, send_sem, recv_sem, peer):
        pltpu.make_async_remote_copy(
            src_ref=src, dst_ref=dst, send_sem=send_sem, recv_sem=recv_sem,
            device_id={"lon": lon, "mem": peer}, device_id_type=MESH,
        ).start()

    def start_runs(chunk):
        parts[chunk] = (total[...] * factor).astype(jnp.bfloat16).reshape(levels, ROWS, width)
        for step in (2, 1, 3):
            peer = (mem_x + step) % n_run
            to_device(
                parts.at[chunk, pl.ds(peer * 2 * levels_out, 2 * levels_out)],
                runs.at[chunk, mem_x], run_send, run_recv.at[chunk], peer * 2 + mem_y,
            )

    def start_half(chunk):
        wait_for(runs.at[chunk, pl.ds(0, n_run - 1)], run_recv.at[chunk])

        def summed(half):
            first = half * levels_out
            value = parts[chunk, pl.ds(mem_x * 2 * levels_out + first, levels_out)].astype(jnp.float32)
            for step in range(1, n_run):
                source = (mem_x + step) % n_run
                value = value + runs[chunk, source, pl.ds(first, levels_out)].astype(jnp.float32)
            return value

        halves[chunk] = summed(1 - mem_y).astype(jnp.bfloat16)
        held[chunk] = summed(mem_y)
        to_device(halves.at[chunk], second.at[chunk], half_send, half_recv.at[chunk], mem_x * 2 + 1 - mem_y)

    def finish(chunk):
        wait_for(second.at[chunk], half_recv.at[chunk])
        out_ref[:, pl.ds(chunk * ROWS, ROWS), :] = held[chunk] + second[chunk].astype(jnp.float32)

    def start_last(peer):
        to_device(
            parts.at[last, pl.ds(peer * levels_out, levels_out)], arrived.at[mem], last_send, last_recv, peer
        )

    def finish_last():
        wait_for(arrived.at[pl.ds(0, n_mem - 1)], last_recv)
        value = parts[last, pl.ds(mem * levels_out, levels_out)].astype(jnp.float32)
        for source in mem_peers:
            value = value + arrived[source].astype(jnp.float32)
        out_ref[:, pl.ds(last * ROWS, ROWS), :] = value

    def landed(chunk, pair):
        wait_for(
            columns.at[chunk, pl.ds(pair * PAIR, PAIR), pl.ds(0, levels - levels_own)],
            recv_sem.at[chunk * pairs + pair],
        )
        return jnp.concatenate(
            [columns[chunk, pair * PAIR + k].reshape(stacked, width) for k in range(PAIR)], axis=1
        )

    def added(value, chunk, pair, both, first_level, n_levels):
        rows = pl.ds(first_level * ROWS, n_levels * ROWS)
        vertical = jnp.dot(kron[rows, :], both, preferred_element_type=jnp.float32).astype(jnp.bfloat16)
        localized = jnp.dot(vertical, lat_two[...], preferred_element_type=jnp.float32)
        for k in range(PAIR):
            pert = perts[chunk, pair * PAIR + k, pl.ds(first_level, n_levels)]
            pert = pert.reshape(n_levels * ROWS, width).astype(jnp.float32)
            value = value + pert * localized[:, k * width : (k + 1) * width]
        return value

    def units_of(chunk, n_pairs):
        own_copy(chunk).wait()
        pert_copy(chunk).wait()
        total[...] = jnp.zeros_like(total)

        def unit_step(pair, carry):

            both = landed(chunk, pair)

            @pl.when((chunk > 0) & (pair == jnp.where(chunk < last, 1, 1 - lon % 2)))
            def _():
                start_half(chunk - 1)

            total[...] = added(total[...], chunk, pair, both, 0, levels)
            return carry

        lax.fori_loop(0, n_pairs, unit_step, 0)

    def chunk_step(chunk, carry):
        units_of(chunk, pairs)
        start_runs(chunk)
        return carry

    lax.fori_loop(0, last, chunk_step, 0)
    units_of(last, pairs)
    own_core = lon % 2

    @pl.when(own_core == 0)
    def _():
        start_runs(last)
        start_half(last)
        for chunk in range(chunks):
            finish(chunk)

    @pl.when(own_core == 1)
    def _():
        parts[last] = (total[...] * factor).astype(jnp.bfloat16).reshape(levels, ROWS, width)
        for step in (2, 1, 3, 0):
            run = (mem_x + step) % n_run
            start_last(run * 2 + 1 - mem_y)
            if step:
                start_last(run * 2 + mem_y)
        for chunk in range(last):
            finish(chunk)
        finish_last()

    wait_for(columns.at[:, :, pl.ds(0, levels - levels_own)], send_sem)
    wait_for(runs.at[pl.ds(0, last), pl.ds(0, n_run - 1)], run_send)
    wait_for(halves.at[pl.ds(0, last)], half_send)

    @pl.when(own_core == 0)
    def _():
        wait_for(runs.at[last, pl.ds(0, n_run - 1)], run_send)
        wait_for(halves.at[last], half_send)

    @pl.when(own_core == 1)
    def _():
        wait_for(arrived.at[pl.ds(0, n_mem - 1)], last_send)


def local(alpha, ens_pert, vert_sqrt, lat_sqrt):
    n_lon, n_mem = lax.axis_size("lon"), lax.axis_size("mem")
    members, levels_own, _, width = alpha.shape
    _, levels, own_rows, _ = ens_pert.shape
    chunks = own_rows // ROWS
    units = chunks * (members // PAIR)
    stacked = levels * ROWS
    levels_out = levels // n_mem
    factor = 1.0 / math.sqrt(members * n_mem)
    hbm = pl.BlockSpec(memory_space=pltpu.HBM)
    half, full = jnp.bfloat16, jnp.float32
    return pl.pallas_call(
        functools.partial(kernel, factor, n_lon, n_mem),
        out_shape=pltpu.VMEM((levels_out, own_rows, width), full),
        in_specs=[hbm] * 4,
        out_specs=pl.BlockSpec(memory_space=pltpu.VMEM),
        scratch_shapes=[
            pltpu.VMEM((chunks, members, levels, ROWS, width), half),
            pltpu.VMEM((chunks, members, levels, ROWS, width), half),
            pltpu.VMEM((PAIR, *alpha.shape[1:]), half),
            pltpu.VMEM((levels, levels), half),
            pltpu.VMEM((stacked, stacked), half),
            pltpu.VMEM((PAIR * width, PAIR * width), half),
            pltpu.VMEM((stacked, width), full),
            pltpu.VMEM((chunks, levels, ROWS, width), half),
            pltpu.VMEM((chunks, n_mem // 2, 2 * levels_out, ROWS, width), half),
            pltpu.VMEM((chunks, levels_out, ROWS, width), full),
            pltpu.VMEM((chunks, levels_out, ROWS, width), half),
            pltpu.VMEM((chunks, levels_out, ROWS, width), half),
            pltpu.VMEM((n_mem, levels_out, ROWS, width), half),
            pltpu.SemaphoreType.DMA,
            pltpu.SemaphoreType.DMA((1 + PAIR,)),
            pltpu.SemaphoreType.DMA((chunks,)),
            pltpu.SemaphoreType.DMA((chunks,)),
            pltpu.SemaphoreType.DMA,
            pltpu.SemaphoreType.DMA((units,)),
            pltpu.SemaphoreType.DMA,
            pltpu.SemaphoreType.DMA((chunks,)),
            pltpu.SemaphoreType.DMA,
            pltpu.SemaphoreType.DMA((chunks,)),
            pltpu.SemaphoreType.DMA,
            pltpu.SemaphoreType.DMA,
        ],
        compiler_params=pltpu.CompilerParams(
            collective_id=0, has_side_effects=True, vmem_limit_bytes=LIMIT * 2**20
        ),
    )(*(pltpu.with_memory_space_constraint(x, pltpu.HBM) for x in (alpha, ens_pert, vert_sqrt, lat_sqrt)))


def solution(mesh):
    placed = (P("mem", "lon", None, None), P("mem", None, "lon", None), P(), P())
    return jax.shard_map(
        local, mesh=mesh, in_specs=placed, out_specs=P("mem", "lon", None), check_vma=False
    )
```

```python
import functools
import math

import jax
import jax.numpy as jnp
from jax import lax
from jax.experimental import pallas as pl
from jax.experimental.pallas import tpu as pltpu
from jax.sharding import PartitionSpec as P

MESH = pl.DeviceIdType.MESH
ROWS = 8
PAIR = 2
HEAD = 2
LIMIT = 54


def kernel(
    factor, n_lon, n_mem, alpha_ref, pert_ref, vert_ref, lat_ref, out_ref,
    columns, perts, staged, vert, kron, lat_two, total, parts, runs, held, halves, second, arrived,
    stage_sem, small_sem, own_sem, pert_sem, send_sem, recv_sem,
    here_sem, run_send, run_recv, half_send, half_recv, last_send, last_recv,
):
    lon, mem = lax.axis_index("lon"), lax.axis_index("mem")
    members, levels_own = alpha_ref.shape[0], alpha_ref.shape[1]
    levels = levels_own * n_lon
    own_rows = pert_ref.shape[2]
    width = lat_ref.shape[0]
    chunks, pairs = own_rows // ROWS, members // PAIR
    units = chunks * pairs
    stacked = levels * ROWS
    levels_out = levels // n_mem
    n_run = n_mem // 2
    mem_x, mem_y = mem // 2, mem % 2
    last = chunks - 1

    def lon_peer(dy, dz, dc):
        y, z, c = lon // 8, (lon // 2) % 4, lon % 2
        return ((y + dy) % 2) * 8 + ((z + dz) % 4) * 2 + (c + dc) % 2

    near = [(1, 0, 0), (1, 0, 1), *((0, dz, dc) for dz in (2, 1, 3) for dc in (0, 1)), (0, 0, 1)]
    far = [(1, dz, dc) for dz in (2, 1, 3) for dc in (0, 1)]
    lon_near = [lon_peer(*offset) for offset in near]
    lon_far = [lon_peer(*offset) for offset in far]
    lon_peers = lon_far + lon_near
    mem_peers = [(mem + step) % n_mem for step in range(1, n_mem)]

    def wait_for(ref, sem):
        pltpu.make_async_copy(ref, ref, sem).wait()

    mem_near = [(mem_x + step) % n_run * 2 + mem_y for step in range(1, n_run)] + [mem_x * 2 + 1 - mem_y]
    barrier = pltpu.get_barrier_semaphore()

    def say(sem, lon_to, mem_to):
        pl.semaphore_signal(sem, inc=1, device_id={"lon": lon_to, "mem": mem_to}, device_id_type=MESH)

    for peer in lon_near:
        say(barrier, peer, mem)
    for peer in mem_near:
        say(barrier, lon, peer)

    def own_copy(chunk):
        rows = pl.ds(pl.multiple_of(lon * own_rows + chunk * ROWS, ROWS), ROWS)
        return pltpu.make_async_copy(
            alpha_ref.at[:, :, rows, :],
            columns.at[chunk, :, pl.ds(lon * levels_own, levels_own)],
            own_sem.at[chunk],
        )

    def pert_copy(chunk):
        rows = pl.ds(pl.multiple_of(chunk * ROWS, ROWS), ROWS)
        return pltpu.make_async_copy(pert_ref.at[:, :, rows, :], perts.at[chunk], pert_sem.at[chunk])

    def send_to(peer, source, unit):
        chunk, group = unit // pairs, pl.ds(unit % pairs * PAIR, PAIR)
        rows = pl.ds(pl.multiple_of(peer * own_rows + chunk * ROWS, ROWS), ROWS)
        pltpu.make_async_remote_copy(
            src_ref=source.at[group, :, rows, :],
            dst_ref=columns.at[chunk, group, pl.ds(lon * levels_own, levels_own)],
            send_sem=send_sem, recv_sem=recv_sem.at[unit],
            device_id={"lon": peer, "mem": mem}, device_id_type=MESH,
        ).start()

    def send_unit(unit, peers, source=alpha_ref):
        for peer in peers:
            send_to(peer, source, unit)

    def send(unit, carry):
        send_unit(unit, lon_peers)
        return carry

    def send_late(core, unit):
        offsets = [(1, 2), (1, 1), (1, 3), (1, 0), (0, 2), (0, 1), (0, 3)]
        send_unit(unit, [lon_peer(dy, dz, core + lon) for dy, dz in offsets])

        @pl.when(lon % 2 != core)
        def _():
            send_unit(unit, [lon_peer(0, 0, 1)])

    stage = pltpu.make_async_copy(alpha_ref.at[pl.ds(0, PAIR)], staged, stage_sem)
    stage.start()
    vert_copy = pltpu.make_async_copy(vert_ref, vert, small_sem.at[0])
    vert_copy.start()
    lat_two[...] = jnp.zeros_like(lat_two)
    stage.wait()
    def head(unit, peers):
        send_unit(unit, peers, staged if unit == 0 else alpha_ref)

    pl.semaphore_wait(barrier, len(lon_near) + len(mem_near))
    say(here_sem, lon_peer(1, 0, 0), mem)
    say(here_sem, lon, mem_x * 2 + 1 - mem_y)
    for unit in range(HEAD):
        head(unit, lon_near)
    pl.semaphore_wait(here_sem, 2)
    for unit in range(HEAD):
        head(unit, lon_far)
    lax.fori_loop(HEAD, last * pairs, send, 0)
    for core in range(2):
        for pair in range(pairs):
            send_late(core, last * pairs + pair)
    lat_copies = [
        pltpu.make_async_copy(
            lat_ref, lat_two.at[pl.ds(k * width, width), pl.ds(k * width, width)], small_sem.at[1 + k]
        )
        for k in range(PAIR)
    ]
    for copy in lat_copies:
        copy.start()
    for chunk in range(chunks):
        own_copy(chunk).start()
        pert_copy(chunk).start()

    wide = (levels, stacked)
    spread = (
        lax.broadcasted_iota(jnp.int32, wide, 1) // ROWS == lax.broadcasted_iota(jnp.int32, wide, 0)
    ).astype(jnp.bfloat16)
    tall = levels // ROWS
    band = (
        lax.broadcasted_iota(jnp.int32, (levels, tall), 0) // ROWS == lax.broadcasted_iota(jnp.int32, (levels, tall), 1)
    ).astype(jnp.bfloat16)
    same = lax.broadcasted_iota(jnp.int32, wide, 0) % ROWS == lax.broadcasted_iota(jnp.int32, wide, 1) % ROWS

    def build(block, carry):
        some = vert[pl.ds(pl.multiple_of(block * tall, tall), tall), :]
        repeated = jnp.dot(band, some, preferred_element_type=jnp.float32).astype(jnp.bfloat16)
        full = jnp.dot(repeated, spread, preferred_element_type=jnp.float32)
        kron[pl.ds(pl.multiple_of(block * levels, levels), levels), :] = jnp.where(same, full, 0.0).astype(jnp.bfloat16)
        return carry

    vert_copy.wait()
    lax.fori_loop(0, stacked // levels, build, 0)
    for copy in lat_copies:
        copy.wait()

    def to_device(src, dst, send_sem, recv_sem, peer):
        pltpu.make_async_remote_copy(
            src_ref=src, dst_ref=dst, send_sem=send_sem, recv_sem=recv_sem,
            device_id={"lon": lon, "mem": peer}, device_id_type=MESH,
        ).start()

    def keep(chunk, value):
        parts[chunk] = (value * factor).astype(jnp.bfloat16).reshape(levels, ROWS, width)

    def start_runs(chunk):
        for step in (2, 1, 3):
            peer = (mem_x + step) % n_run
            to_device(
                parts.at[chunk, pl.ds(peer * 2 * levels_out, 2 * levels_out)],
                runs.at[chunk, mem_x], run_send, run_recv.at[chunk], peer * 2 + mem_y,
            )

    def start_half(chunk):
        wait_for(runs.at[chunk, pl.ds(0, n_run - 1)], run_recv.at[chunk])

        def summed(half):
            first = half * levels_out
            value = parts[chunk, pl.ds(mem_x * 2 * levels_out + first, levels_out)].astype(jnp.float32)
            for step in range(1, n_run):
                source = (mem_x + step) % n_run
                value = value + runs[chunk, source, pl.ds(first, levels_out)].astype(jnp.float32)
            return value

        halves[chunk] = summed(1 - mem_y).astype(jnp.bfloat16)
        held[chunk] = summed(mem_y)
        to_device(halves.at[chunk], second.at[chunk], half_send, half_recv.at[chunk], mem_x * 2 + 1 - mem_y)

    def finish(chunk):
        wait_for(second.at[chunk], half_recv.at[chunk])
        out_ref[:, pl.ds(chunk * ROWS, ROWS), :] = held[chunk] + second[chunk].astype(jnp.float32)

    def start_last(peer):
        to_device(
            parts.at[last, pl.ds(peer * levels_out, levels_out)], arrived.at[mem], last_send, last_recv, peer
        )

    def finish_last():
        wait_for(arrived.at[pl.ds(0, n_mem - 1)], last_recv)
        value = parts[last, pl.ds(mem * levels_out, levels_out)].astype(jnp.float32)
        for source in mem_peers:
            value = value + arrived[source].astype(jnp.float32)
        out_ref[:, pl.ds(last * ROWS, ROWS), :] = value

    def added(value, chunk, pair):
        first = pair * PAIR
        wait_for(
            columns.at[chunk, pl.ds(first, PAIR), pl.ds(0, levels - levels_own)], recv_sem.at[chunk * pairs + pair]
        )
        fields = jnp.concatenate([columns[chunk, first + k].reshape(stacked, width) for k in range(PAIR)], axis=1)
        vertical = jnp.dot(kron[...], fields, preferred_element_type=jnp.float32).astype(jnp.bfloat16)
        localized = jnp.dot(vertical, lat_two[...], preferred_element_type=jnp.float32)
        for k in range(PAIR):
            pert = perts[chunk, first + k].reshape(stacked, width).astype(jnp.float32)
            value = value + pert * localized[:, k * width : (k + 1) * width]
        return value

    def units_of(chunk, n_pairs):
        own_copy(chunk).wait()
        pert_copy(chunk).wait()
        total[...] = jnp.zeros_like(total)

        def unit_step(pair, carry):

            total[...] = added(total[...], chunk, pair)

            @pl.when((chunk > 0) & (pair == jnp.where(chunk < last, 1, 1 - lon % 2)))
            def _():
                start_half(chunk - 1)

            return carry

        lax.fori_loop(0, n_pairs, unit_step, 0)

    def chunk_step(chunk, carry):
        units_of(chunk, pairs)
        keep(chunk, total[...])
        start_runs(chunk)
        return carry

    lax.fori_loop(0, last, chunk_step, 0)
    units_of(last, pairs)
    keep(last, total[...])
    own_core = lon % 2

    @pl.when(own_core == 0)
    def _():
        start_runs(last)
        start_half(last)
        for chunk in range(chunks):
            finish(chunk)

    @pl.when(own_core == 1)
    def _():
        for step in (2, 1, 3, 0):
            run = (mem_x + step) % n_run
            start_last(run * 2 + 1 - mem_y)
            if step:
                start_last(run * 2 + mem_y)
        for chunk in range(last):
            finish(chunk)
        finish_last()

    wait_for(columns.at[:, :, pl.ds(0, levels - levels_own)], send_sem)
    wait_for(runs.at[pl.ds(0, last), pl.ds(0, n_run - 1)], run_send)
    wait_for(halves.at[pl.ds(0, last)], half_send)

    @pl.when(own_core == 0)
    def _():
        wait_for(runs.at[last, pl.ds(0, n_run - 1)], run_send)
        wait_for(halves.at[last], half_send)

    @pl.when(own_core == 1)
    def _():
        wait_for(arrived.at[pl.ds(0, n_mem - 1)], last_send)


def local(alpha, ens_pert, vert_sqrt, lat_sqrt):
    n_lon, n_mem = lax.axis_size("lon"), lax.axis_size("mem")
    members, levels_own, _, width = alpha.shape
    _, levels, own_rows, _ = ens_pert.shape
    chunks = own_rows // ROWS
    units = chunks * (members // PAIR)
    stacked = levels * ROWS
    levels_out = levels // n_mem
    factor = 1.0 / math.sqrt(members * n_mem)
    hbm = pl.BlockSpec(memory_space=pltpu.HBM)
    half, full = jnp.bfloat16, jnp.float32
    return pl.pallas_call(
        functools.partial(kernel, factor, n_lon, n_mem),
        out_shape=pltpu.VMEM((levels_out, own_rows, width), full),
        in_specs=[hbm] * 4,
        out_specs=pl.BlockSpec(memory_space=pltpu.VMEM),
        scratch_shapes=[
            pltpu.VMEM((chunks, members, levels, ROWS, width), half),
            pltpu.VMEM((chunks, members, levels, ROWS, width), half),
            pltpu.VMEM((PAIR, *alpha.shape[1:]), half),
            pltpu.VMEM((levels, levels), half),
            pltpu.VMEM((stacked, stacked), half),
            pltpu.VMEM((PAIR * width, PAIR * width), half),
            pltpu.VMEM((stacked, width), full),
            pltpu.VMEM((chunks, levels, ROWS, width), half),
            pltpu.VMEM((chunks, n_mem // 2, 2 * levels_out, ROWS, width), half),
            pltpu.VMEM((chunks, levels_out, ROWS, width), full),
            pltpu.VMEM((chunks, levels_out, ROWS, width), half),
            pltpu.VMEM((chunks, levels_out, ROWS, width), half),
            pltpu.VMEM((n_mem, levels_out, ROWS, width), half),
            pltpu.SemaphoreType.DMA,
            pltpu.SemaphoreType.DMA((1 + PAIR,)),
            pltpu.SemaphoreType.DMA((chunks,)),
            pltpu.SemaphoreType.DMA((chunks,)),
            pltpu.SemaphoreType.DMA,
            pltpu.SemaphoreType.DMA((units,)),
            pltpu.SemaphoreType.REGULAR,
            pltpu.SemaphoreType.DMA,
            pltpu.SemaphoreType.DMA((chunks,)),
            pltpu.SemaphoreType.DMA,
            pltpu.SemaphoreType.DMA((chunks,)),
            pltpu.SemaphoreType.DMA,
            pltpu.SemaphoreType.DMA,
        ],
        compiler_params=pltpu.CompilerParams(
            collective_id=0, has_side_effects=True, vmem_limit_bytes=LIMIT * 2**20
        ),
    )(*(pltpu.with_memory_space_constraint(x, pltpu.HBM) for x in (alpha, ens_pert, vert_sqrt, lat_sqrt)))


def solution(mesh):
    placed = (P("mem", "lon", None, None), P("mem", None, "lon", None), P(), P())
    return jax.shard_map(
        local, mesh=mesh, in_specs=placed, out_specs=P("mem", "lon", None), check_vma=False
    )
```

```python
import functools
import math

import jax
import jax.numpy as jnp
from jax import lax
from jax.experimental import pallas as pl
from jax.experimental.pallas import tpu as pltpu
from jax.sharding import PartitionSpec as P

MESH = pl.DeviceIdType.MESH
ROWS = 8
PAIR = 2
HEAD = 2
FLAGS = {}
LIMIT = 54


def kernel(
    factor, n_lon, n_mem, alpha_ref, pert_ref, vert_ref, lat_ref, out_ref,
    columns, perts, staged, vert, kron, lat_two, total, partial, parts, runs, held, halves, second, arrived,
    stage_sem, small_sem, own_sem, pert_sem, send_sem, recv_sem,
    here_sem, run_send, run_recv, half_send, half_recv, last_send, last_recv,
):
    lon, mem = lax.axis_index("lon"), lax.axis_index("mem")
    members, levels_own = alpha_ref.shape[0], alpha_ref.shape[1]
    levels = levels_own * n_lon
    own_rows = pert_ref.shape[2]
    width = lat_ref.shape[0]
    chunks, pairs = own_rows // ROWS, members // PAIR
    units = chunks * pairs
    stacked = levels * ROWS
    levels_out = levels // n_mem
    n_run = n_mem // 2
    mem_x, mem_y = mem // 2, mem % 2
    last = chunks - 1

    def lon_peer(dy, dz, dc):
        y, z, c = lon // 8, (lon // 2) % 4, lon % 2
        return ((y + dy) % 2) * 8 + ((z + dz) % 4) * 2 + (c + dc) % 2

    near = [(1, 0, 0), (1, 0, 1), *((0, dz, dc) for dz in (2, 1, 3) for dc in (0, 1)), (0, 0, 1)]
    far = [(1, dz, dc) for dz in (2, 1, 3) for dc in (0, 1)]
    lon_near = [lon_peer(*offset) for offset in near]
    lon_far = [lon_peer(*offset) for offset in far]
    lon_peers = lon_far + lon_near
    mem_peers = [(mem + step) % n_mem for step in range(1, n_mem)]

    def wait_for(ref, sem):
        pltpu.make_async_copy(ref, ref, sem).wait()

    mem_near = [(mem_x + step) % n_run * 2 + mem_y for step in range(1, n_run)] + [mem_x * 2 + 1 - mem_y]
    barrier = pltpu.get_barrier_semaphore()

    def say(sem, lon_to, mem_to):
        pl.semaphore_signal(sem, inc=1, device_id={"lon": lon_to, "mem": mem_to}, device_id_type=MESH)

    for peer in lon_near:
        say(barrier, peer, mem)
    for peer in mem_near:
        say(barrier, lon, peer)

    def own_copy(chunk):
        rows = pl.ds(pl.multiple_of(lon * own_rows + chunk * ROWS, ROWS), ROWS)
        return pltpu.make_async_copy(
            alpha_ref.at[:, :, rows, :],
            columns.at[chunk, :, pl.ds(lon * levels_own, levels_own)],
            own_sem.at[chunk],
        )

    def pert_copy(chunk):
        rows = pl.ds(pl.multiple_of(chunk * ROWS, ROWS), ROWS)
        return pltpu.make_async_copy(pert_ref.at[:, :, rows, :], perts.at[chunk], pert_sem.at[chunk])

    def send_to(peer, source, unit, sem):
        chunk, group = unit // pairs, pl.ds(unit % pairs * PAIR, PAIR)
        rows = pl.ds(pl.multiple_of(peer * own_rows + chunk * ROWS, ROWS), ROWS)
        pltpu.make_async_remote_copy(
            src_ref=source.at[group, :, rows, :],
            dst_ref=columns.at[chunk, group, pl.ds(lon * levels_own, levels_own)],
            send_sem=send_sem, recv_sem=recv_sem.at[unit] if sem is None else sem,
            device_id={"lon": peer, "mem": mem}, device_id_type=MESH,
        ).start()

    def send_unit(unit, peers, source=alpha_ref, sem=None):
        for peer in peers:
            send_to(peer, source, unit, sem)

    def send(unit, carry):
        send_unit(unit, lon_peers)
        return carry

    def send_late(core, unit, sides=(1, 0), sem=None):
        offsets = [(1, 2), (1, 1), (1, 3), (1, 0), (0, 2), (0, 1), (0, 3)]
        send_unit(unit, [lon_peer(dy, dz, core + lon) for dy, dz in offsets if dy in sides], sem=sem)
        if 0 in sides:
            @pl.when(lon % 2 != core)
            def _():
                send_unit(unit, [lon_peer(0, 0, 1)])

    stage = pltpu.make_async_copy(alpha_ref.at[pl.ds(0, PAIR)], staged, stage_sem)
    stage.start()
    vert_copy = pltpu.make_async_copy(vert_ref, vert, small_sem.at[0])
    vert_copy.start()
    lat_two[...] = jnp.zeros_like(lat_two)
    stage.wait()
    def head(unit, peers):
        send_unit(unit, peers, staged if unit == 0 else alpha_ref)

    pl.semaphore_wait(barrier, len(lon_near) + len(mem_near))
    say(here_sem, lon_peer(1, 0, 0), mem)
    say(here_sem, lon, mem_x * 2 + 1 - mem_y)
    for unit in range(HEAD):
        head(unit, lon_near)
    pl.semaphore_wait(here_sem, 2)
    for unit in range(HEAD):
        head(unit, lon_far)
    lax.fori_loop(HEAD, last * pairs, send, 0)
    for core in range(2):
        for pair in range(pairs - 1):
            send_late(core, last * pairs + pair)
        send_late(core, units - 1, (0,))
        send_late(core, units - 1, (1,), recv_sem.at[units])
    lat_copies = [
        pltpu.make_async_copy(
            lat_ref, lat_two.at[pl.ds(k * width, width), pl.ds(k * width, width)], small_sem.at[1 + k]
        )
        for k in range(PAIR)
    ]
    for copy in lat_copies:
        copy.start()
    for chunk in range(chunks):
        own_copy(chunk).start()
        pert_copy(chunk).start()

    wide = (levels, stacked)
    spread = (
        lax.broadcasted_iota(jnp.int32, wide, 1) // ROWS == lax.broadcasted_iota(jnp.int32, wide, 0)
    ).astype(jnp.bfloat16)
    tall = levels // ROWS
    band = (
        lax.broadcasted_iota(jnp.int32, (levels, tall), 0) // ROWS == lax.broadcasted_iota(jnp.int32, (levels, tall), 1)
    ).astype(jnp.bfloat16)
    same = lax.broadcasted_iota(jnp.int32, wide, 0) % ROWS == lax.broadcasted_iota(jnp.int32, wide, 1) % ROWS

    def build(block, carry):
        some = vert[pl.ds(pl.multiple_of(block * tall, tall), tall), :]
        repeated = jnp.dot(band, some, preferred_element_type=jnp.float32).astype(jnp.bfloat16)
        full = jnp.dot(repeated, spread, preferred_element_type=jnp.float32)
        kron[pl.ds(pl.multiple_of(block * levels, levels), levels), :] = jnp.where(same, full, 0.0).astype(jnp.bfloat16)
        return carry

    vert_copy.wait()
    lax.fori_loop(0, stacked // levels, build, 0)
    for copy in lat_copies:
        copy.wait()

    def to_device(src, dst, send_sem, recv_sem, peer):
        pltpu.make_async_remote_copy(
            src_ref=src, dst_ref=dst, send_sem=send_sem, recv_sem=recv_sem,
            device_id={"lon": lon, "mem": peer}, device_id_type=MESH,
        ).start()

    def keep(chunk, value):
        parts[chunk] = (value * factor).astype(jnp.bfloat16).reshape(levels, ROWS, width)

    def start_runs(chunk):
        for step in (2, 1, 3):
            peer = (mem_x + step) % n_run
            to_device(
                parts.at[chunk, pl.ds(peer * 2 * levels_out, 2 * levels_out)],
                runs.at[chunk, mem_x], run_send, run_recv.at[chunk], peer * 2 + mem_y,
            )

    def start_half(chunk):
        wait_for(runs.at[chunk, pl.ds(0, n_run - 1)], run_recv.at[chunk])

        def summed(half):
            first = half * levels_out
            value = parts[chunk, pl.ds(mem_x * 2 * levels_out + first, levels_out)].astype(jnp.float32)
            for step in range(1, n_run):
                source = (mem_x + step) % n_run
                value = value + runs[chunk, source, pl.ds(first, levels_out)].astype(jnp.float32)
            return value

        halves[chunk] = summed(1 - mem_y).astype(jnp.bfloat16)
        held[chunk] = summed(mem_y)
        to_device(halves.at[chunk], second.at[chunk], half_send, half_recv.at[chunk], mem_x * 2 + 1 - mem_y)

    def finish(chunk):
        wait_for(second.at[chunk], half_recv.at[chunk])
        out_ref[:, pl.ds(chunk * ROWS, ROWS), :] = held[chunk] + second[chunk].astype(jnp.float32)

    def start_last(peer):
        to_device(
            parts.at[last, pl.ds(peer * levels_out, levels_out)], arrived.at[mem], last_send, last_recv, peer
        )

    def finish_last():
        wait_for(arrived.at[pl.ds(0, n_mem - 1)], last_recv)
        value = parts[last, pl.ds(mem * levels_out, levels_out)].astype(jnp.float32)
        for source in mem_peers:
            value = value + arrived[source].astype(jnp.float32)
        out_ref[:, pl.ds(last * ROWS, ROWS), :] = value

    def added(value, chunk, pair):
        first = pair * PAIR
        wait_for(
            columns.at[chunk, pl.ds(first, PAIR), pl.ds(0, levels - levels_own)], recv_sem.at[chunk * pairs + pair]
        )
        fields = jnp.concatenate([columns[chunk, first + k].reshape(stacked, width) for k in range(PAIR)], axis=1)
        vertical = jnp.dot(kron[...], fields, preferred_element_type=jnp.float32).astype(jnp.bfloat16)
        localized = jnp.dot(vertical, lat_two[...], preferred_element_type=jnp.float32)
        for k in range(PAIR):
            pert = perts[chunk, first + k].reshape(stacked, width).astype(jnp.float32)
            value = value + pert * localized[:, k * width : (k + 1) * width]
        return value

    def units_of(chunk, n_pairs):
        own_copy(chunk).wait()
        pert_copy(chunk).wait()
        total[...] = jnp.zeros_like(total)

        def unit_step(pair, carry):

            total[...] = added(total[...], chunk, pair)

            @pl.when((chunk > 0) & (pair == jnp.where(chunk < last, 1, 1 - lon % 2)))
            def _():
                start_half(chunk - 1)

            return carry

        lax.fori_loop(0, n_pairs, unit_step, 0)

    def chunk_step(chunk, carry):
        units_of(chunk, pairs)
        keep(chunk, total[...])
        start_runs(chunk)
        return carry

    lax.fori_loop(0, last, chunk_step, 0)
    units_of(last, pairs - 1)
    side = lon // (n_lon // 2)
    half = levels // 2
    first = members - PAIR
    group = pl.ds(first, PAIR)

    def half_of(side):
        levels_of = pl.ds(pl.multiple_of(side * half, half), half)
        fields = [columns[last, first + k, levels_of].reshape(half * ROWS, width) for k in range(PAIR)]
        across = pl.ds(pl.multiple_of(side * half * ROWS, half * ROWS), half * ROWS)
        return jnp.dot(kron[:, across], jnp.concatenate(fields, axis=1), preferred_element_type=jnp.float32)

    wait_for(columns.at[last, group, pl.ds(0, half - levels_own)], recv_sem.at[units - 1])
    partial[...] = half_of(side)
    wait_for(columns.at[last, group, pl.ds(0, half)], recv_sem.at[units])
    vertical = (partial[...] + half_of(1 - side)).astype(jnp.bfloat16)
    localized = jnp.dot(vertical, lat_two[...], preferred_element_type=jnp.float32)
    value = total[...]
    for k in range(PAIR):
        pert = perts[last, first + k].reshape(stacked, width).astype(jnp.float32)
        value = value + pert * localized[:, k * width : (k + 1) * width]
    keep(last, value)
    own_core = lon % 2

    @pl.when(own_core == 0)
    def _():
        start_runs(last)
        start_half(last)
        for chunk in range(chunks):
            finish(chunk)

    @pl.when(own_core == 1)
    def _():
        for step in (2, 1, 3, 0):
            run = (mem_x + step) % n_run
            start_last(run * 2 + 1 - mem_y)
            if step:
                start_last(run * 2 + mem_y)
        for chunk in range(last):
            finish(chunk)
        finish_last()

    wait_for(columns.at[:, :, pl.ds(0, levels - levels_own)], send_sem)
    wait_for(runs.at[pl.ds(0, last), pl.ds(0, n_run - 1)], run_send)
    wait_for(halves.at[pl.ds(0, last)], half_send)

    @pl.when(own_core == 0)
    def _():
        wait_for(runs.at[last, pl.ds(0, n_run - 1)], run_send)
        wait_for(halves.at[last], half_send)

    @pl.when(own_core == 1)
    def _():
        wait_for(arrived.at[pl.ds(0, n_mem - 1)], last_send)


def local(alpha, ens_pert, vert_sqrt, lat_sqrt):
    n_lon, n_mem = lax.axis_size("lon"), lax.axis_size("mem")
    members, levels_own, _, width = alpha.shape
    _, levels, own_rows, _ = ens_pert.shape
    chunks = own_rows // ROWS
    units = chunks * (members // PAIR)
    stacked = levels * ROWS
    levels_out = levels // n_mem
    factor = 1.0 / math.sqrt(members * n_mem)
    hbm = pl.BlockSpec(memory_space=pltpu.HBM)
    half, full = jnp.bfloat16, jnp.float32
    return pl.pallas_call(
        functools.partial(kernel, factor, n_lon, n_mem),
        out_shape=pltpu.VMEM((levels_out, own_rows, width), full),
        in_specs=[hbm] * 4,
        out_specs=pl.BlockSpec(memory_space=pltpu.VMEM),
        scratch_shapes=[
            pltpu.VMEM((chunks, members, levels, ROWS, width), half),
            pltpu.VMEM((chunks, members, levels, ROWS, width), half),
            pltpu.VMEM((PAIR, *alpha.shape[1:]), half),
            pltpu.VMEM((levels, levels), half),
            pltpu.VMEM((stacked, stacked), half),
            pltpu.VMEM((PAIR * width, PAIR * width), half),
            pltpu.VMEM((stacked, width), full),
            pltpu.VMEM((stacked, PAIR * width), full),
            pltpu.VMEM((chunks, levels, ROWS, width), half),
            pltpu.VMEM((chunks, n_mem // 2, 2 * levels_out, ROWS, width), half),
            pltpu.VMEM((chunks, levels_out, ROWS, width), full),
            pltpu.VMEM((chunks, levels_out, ROWS, width), half),
            pltpu.VMEM((chunks, levels_out, ROWS, width), half),
            pltpu.VMEM((n_mem, levels_out, ROWS, width), half),
            pltpu.SemaphoreType.DMA,
            pltpu.SemaphoreType.DMA((1 + PAIR,)),
            pltpu.SemaphoreType.DMA((chunks,)),
            pltpu.SemaphoreType.DMA((chunks,)),
            pltpu.SemaphoreType.DMA,
            pltpu.SemaphoreType.DMA((units + 1,)),
            pltpu.SemaphoreType.REGULAR,
            pltpu.SemaphoreType.DMA,
            pltpu.SemaphoreType.DMA((chunks,)),
            pltpu.SemaphoreType.DMA,
            pltpu.SemaphoreType.DMA((chunks,)),
            pltpu.SemaphoreType.DMA,
            pltpu.SemaphoreType.DMA,
        ],
        compiler_params=pltpu.CompilerParams(
            collective_id=0, has_side_effects=True, flags=FLAGS, vmem_limit_bytes=LIMIT * 2**20
        ),
    )(*(pltpu.with_memory_space_constraint(x, pltpu.HBM) for x in (alpha, ens_pert, vert_sqrt, lat_sqrt)))


def solution(mesh):
    placed = (P("mem", "lon", None, None), P("mem", None, "lon", None), P(), P())
    return jax.shard_map(
        local, mesh=mesh, in_specs=placed, out_specs=P("mem", "lon", None), check_vma=False
    )
```

```python
import functools
import math

import jax
import jax.numpy as jnp
from jax import lax
from jax.experimental import pallas as pl
from jax.experimental.pallas import tpu as pltpu
from jax.sharding import PartitionSpec as P

MESH = pl.DeviceIdType.MESH
ROWS = 8
PAIR = 2
HEAD = 2
FLAGS = {}
LIMIT = 54


def kernel(
    factor, n_lon, n_mem, alpha_ref, pert_ref, vert_ref, lat_ref, out_ref,
    columns, perts, staged, vert, kron, lat_two, total, partial, whole, parts, runs, held, halves, second, arrived,
    stage_sem, small_sem, own_sem, pert_sem, send_sem, recv_sem,
    here_sem, run_send, run_recv, half_send, half_recv, last_send, last_recv,
):
    lon, mem = lax.axis_index("lon"), lax.axis_index("mem")
    members, levels_own = alpha_ref.shape[0], alpha_ref.shape[1]
    levels = levels_own * n_lon
    own_rows = pert_ref.shape[2]
    width = lat_ref.shape[0]
    chunks, pairs = own_rows // ROWS, members // PAIR
    units = chunks * pairs
    stacked = levels * ROWS
    levels_out = levels // n_mem
    n_run = n_mem // 2
    mem_x, mem_y = mem // 2, mem % 2
    last = chunks - 1

    def lon_peer(dy, dz, dc):
        y, z, c = lon // 8, (lon // 2) % 4, lon % 2
        return ((y + dy) % 2) * 8 + ((z + dz) % 4) * 2 + (c + dc) % 2

    near = [(1, 0, 0), (1, 0, 1), *((0, dz, dc) for dz in (2, 1, 3) for dc in (0, 1)), (0, 0, 1)]
    far = [(1, dz, dc) for dz in (2, 1, 3) for dc in (0, 1)]
    lon_near = [lon_peer(*offset) for offset in near]
    lon_far = [lon_peer(*offset) for offset in far]
    lon_peers = lon_far + lon_near
    mem_peers = [(mem + step) % n_mem for step in range(1, n_mem)]

    def wait_for(ref, sem):
        pltpu.make_async_copy(ref, ref, sem).wait()

    mem_near = [(mem_x + step) % n_run * 2 + mem_y for step in range(1, n_run)] + [mem_x * 2 + 1 - mem_y]
    barrier = pltpu.get_barrier_semaphore()

    def say(sem, lon_to, mem_to):
        pl.semaphore_signal(sem, inc=1, device_id={"lon": lon_to, "mem": mem_to}, device_id_type=MESH)

    for peer in lon_near:
        say(barrier, peer, mem)
    for peer in mem_near:
        say(barrier, lon, peer)

    def own_copy(chunk):
        rows = pl.ds(pl.multiple_of(lon * own_rows + chunk * ROWS, ROWS), ROWS)
        return pltpu.make_async_copy(
            alpha_ref.at[:, :, rows, :],
            columns.at[chunk, :, pl.ds(lon * levels_own, levels_own)],
            own_sem.at[chunk],
        )

    def pert_copy(chunk):
        rows = pl.ds(pl.multiple_of(chunk * ROWS, ROWS), ROWS)
        return pltpu.make_async_copy(pert_ref.at[:, :, rows, :], perts.at[chunk], pert_sem.at[chunk])

    def send_to(peer, source, unit, sem):
        chunk, group = unit // pairs, pl.ds(unit % pairs * PAIR, PAIR)
        rows = pl.ds(pl.multiple_of(peer * own_rows + chunk * ROWS, ROWS), ROWS)
        pltpu.make_async_remote_copy(
            src_ref=source.at[group, :, rows, :],
            dst_ref=columns.at[chunk, group, pl.ds(lon * levels_own, levels_own)],
            send_sem=send_sem, recv_sem=recv_sem.at[unit] if sem is None else sem,
            device_id={"lon": peer, "mem": mem}, device_id_type=MESH,
        ).start()

    def send_unit(unit, peers, source=alpha_ref, sem=None):
        for peer in peers:
            send_to(peer, source, unit, sem)

    def send(unit, carry):
        send_unit(unit, lon_peers)
        return carry

    def send_late(core, unit, sides=(1, 0), sem=None):
        offsets = [(1, 2), (1, 1), (1, 3), (1, 0), (0, 2), (0, 1), (0, 3)]
        send_unit(unit, [lon_peer(dy, dz, core + lon) for dy, dz in offsets if dy in sides], sem=sem)
        if 0 in sides:
            @pl.when(lon % 2 != core)
            def _():
                send_unit(unit, [lon_peer(0, 0, 1)])

    stage = pltpu.make_async_copy(alpha_ref.at[pl.ds(0, PAIR)], staged, stage_sem)
    stage.start()
    vert_copy = pltpu.make_async_copy(vert_ref, vert, small_sem.at[0])
    vert_copy.start()
    lat_two[...] = jnp.zeros_like(lat_two)
    stage.wait()
    def head(unit, peers):
        send_unit(unit, peers, staged if unit == 0 else alpha_ref)

    pl.semaphore_wait(barrier, len(lon_near) + len(mem_near))
    say(here_sem, lon_peer(1, 0, 0), mem)
    say(here_sem, lon, mem_x * 2 + 1 - mem_y)
    for unit in range(HEAD):
        head(unit, lon_near)
    pl.semaphore_wait(here_sem, 2)
    for unit in range(HEAD):
        head(unit, lon_far)
    lax.fori_loop(HEAD, last * pairs, send, 0)
    for core in range(2):
        for pair in range(pairs - 1):
            send_late(core, last * pairs + pair)
        send_late(core, units - 1, (0,))
        send_late(core, units - 1, (1,), recv_sem.at[units])
    lat_copies = [
        pltpu.make_async_copy(
            lat_ref, lat_two.at[pl.ds(k * width, width), pl.ds(k * width, width)], small_sem.at[1 + k]
        )
        for k in range(PAIR)
    ]
    for copy in lat_copies:
        copy.start()
    for chunk in range(chunks):
        own_copy(chunk).start()
        pert_copy(chunk).start()

    wide = (levels, stacked)
    spread = (
        lax.broadcasted_iota(jnp.int32, wide, 1) // ROWS == lax.broadcasted_iota(jnp.int32, wide, 0)
    ).astype(jnp.bfloat16)
    tall = levels // ROWS
    band = (
        lax.broadcasted_iota(jnp.int32, (levels, tall), 0) // ROWS == lax.broadcasted_iota(jnp.int32, (levels, tall), 1)
    ).astype(jnp.bfloat16)
    same = lax.broadcasted_iota(jnp.int32, wide, 0) % ROWS == lax.broadcasted_iota(jnp.int32, wide, 1) % ROWS

    def build(block, carry):
        some = vert[pl.ds(pl.multiple_of(block * tall, tall), tall), :]
        repeated = jnp.dot(band, some, preferred_element_type=jnp.float32).astype(jnp.bfloat16)
        full = jnp.dot(repeated, spread, preferred_element_type=jnp.float32)
        kron[pl.ds(pl.multiple_of(block * levels, levels), levels), :] = jnp.where(same, full, 0.0).astype(jnp.bfloat16)
        return carry

    vert_copy.wait()
    lax.fori_loop(0, stacked // levels, build, 0)
    for copy in lat_copies:
        copy.wait()

    def to_device(src, dst, send_sem, recv_sem, peer):
        pltpu.make_async_remote_copy(
            src_ref=src, dst_ref=dst, send_sem=send_sem, recv_sem=recv_sem,
            device_id={"lon": lon, "mem": peer}, device_id_type=MESH,
        ).start()

    def keep(chunk, value):
        parts[chunk] = (value * factor).astype(jnp.bfloat16).reshape(levels, ROWS, width)

    def start_runs(chunk):
        for step in (2, 1, 3):
            peer = (mem_x + step) % n_run
            to_device(
                parts.at[chunk, pl.ds(peer * 2 * levels_out, 2 * levels_out)],
                runs.at[chunk, mem_x], run_send, run_recv.at[chunk], peer * 2 + mem_y,
            )

    def start_half(chunk):
        wait_for(runs.at[chunk, pl.ds(0, n_run - 1)], run_recv.at[chunk])

        def summed(half):
            first = half * levels_out
            value = parts[chunk, pl.ds(mem_x * 2 * levels_out + first, levels_out)].astype(jnp.float32)
            for step in range(1, n_run):
                source = (mem_x + step) % n_run
                value = value + runs[chunk, source, pl.ds(first, levels_out)].astype(jnp.float32)
            return value

        halves[chunk] = summed(1 - mem_y).astype(jnp.bfloat16)
        held[chunk] = summed(mem_y)
        to_device(halves.at[chunk], second.at[chunk], half_send, half_recv.at[chunk], mem_x * 2 + 1 - mem_y)

    def finish(chunk):
        wait_for(second.at[chunk], half_recv.at[chunk])
        out_ref[:, pl.ds(chunk * ROWS, ROWS), :] = held[chunk] + second[chunk].astype(jnp.float32)

    def start_last(peer):
        to_device(
            parts.at[last, pl.ds(peer * levels_out, levels_out)], arrived.at[mem], last_send, last_recv, peer
        )

    def finish_last():
        wait_for(arrived.at[pl.ds(0, n_mem - 1)], last_recv)
        value = parts[last, pl.ds(mem * levels_out, levels_out)].astype(jnp.float32)
        for source in mem_peers:
            value = value + arrived[source].astype(jnp.float32)
        out_ref[:, pl.ds(last * ROWS, ROWS), :] = value

    def added(value, chunk, pair):
        first = pair * PAIR
        wait_for(
            columns.at[chunk, pl.ds(first, PAIR), pl.ds(0, levels - levels_own)], recv_sem.at[chunk * pairs + pair]
        )
        fields = jnp.concatenate([columns[chunk, first + k].reshape(stacked, width) for k in range(PAIR)], axis=1)
        vertical = jnp.dot(kron[...], fields, preferred_element_type=jnp.float32).astype(jnp.bfloat16)
        localized = jnp.dot(vertical, lat_two[...], preferred_element_type=jnp.float32)
        for k in range(PAIR):
            pert = perts[chunk, first + k].reshape(stacked, width).astype(jnp.float32)
            value = value + pert * localized[:, k * width : (k + 1) * width]
        return value

    def units_of(chunk, n_pairs):
        own_copy(chunk).wait()
        pert_copy(chunk).wait()
        total[...] = jnp.zeros_like(total)

        def unit_step(pair, carry):

            total[...] = added(total[...], chunk, pair)

            @pl.when((chunk > 0) & (pair == jnp.where(chunk < last, 1, 1 - lon % 2)))
            def _():
                start_half(chunk - 1)

            return carry

        lax.fori_loop(0, n_pairs, unit_step, 0)

    def chunk_step(chunk, carry):
        units_of(chunk, pairs)
        keep(chunk, total[...])
        start_runs(chunk)
        return carry

    lax.fori_loop(0, last, chunk_step, 0)
    units_of(last, pairs - 1)
    side = lon // (n_lon // 2)
    half = levels // 2
    first = members - PAIR
    group = pl.ds(first, PAIR)

    def half_of(side):
        levels_of = pl.ds(pl.multiple_of(side * half, half), half)
        fields = [columns[last, first + k, levels_of].reshape(half * ROWS, width) for k in range(PAIR)]
        across = pl.ds(pl.multiple_of(side * half * ROWS, half * ROWS), half * ROWS)
        return jnp.dot(kron[:, across], jnp.concatenate(fields, axis=1), preferred_element_type=jnp.float32)

    wait_for(columns.at[last, group, pl.ds(0, half - levels_own)], recv_sem.at[units - 1])
    partial[...] = half_of(side)
    wait_for(columns.at[last, group, pl.ds(0, half)], recv_sem.at[units])
    whole[...] = (partial[...] + half_of(1 - side)).astype(jnp.bfloat16)
    of_run = 2 * levels_out
    for step in (2, 1, 3, 0):
        run = (mem_x + step) % n_run
        levels_of = pl.ds(pl.multiple_of(run * of_run, of_run), of_run)
        rows = pl.ds(pl.multiple_of(run * of_run * ROWS, of_run * ROWS), of_run * ROWS)
        localized = jnp.dot(whole[rows, :], lat_two[...], preferred_element_type=jnp.float32)
        value = total[rows, :]
        for k in range(PAIR):
            pert = perts[last, first + k, levels_of].reshape(of_run * ROWS, width).astype(jnp.float32)
            value = value + pert * localized[:, k * width : (k + 1) * width]
        parts[last, levels_of] = (value * factor).astype(jnp.bfloat16).reshape(of_run, ROWS, width)

        @pl.when(lon % 2 == 1)
        def _():
            start_last(run * 2 + 1 - mem_y)
            if step:
                start_last(run * 2 + mem_y)

    own_core = lon % 2

    @pl.when(own_core == 0)
    def _():
        start_runs(last)
        start_half(last)
        for chunk in range(chunks):
            finish(chunk)

    @pl.when(own_core == 1)
    def _():
        for chunk in range(last):
            finish(chunk)
        finish_last()

    wait_for(columns.at[:, :, pl.ds(0, levels - levels_own)], send_sem)
    wait_for(runs.at[pl.ds(0, last), pl.ds(0, n_run - 1)], run_send)
    wait_for(halves.at[pl.ds(0, last)], half_send)

    @pl.when(own_core == 0)
    def _():
        wait_for(runs.at[last, pl.ds(0, n_run - 1)], run_send)
        wait_for(halves.at[last], half_send)

    @pl.when(own_core == 1)
    def _():
        wait_for(arrived.at[pl.ds(0, n_mem - 1)], last_send)


def local(alpha, ens_pert, vert_sqrt, lat_sqrt):
    n_lon, n_mem = lax.axis_size("lon"), lax.axis_size("mem")
    members, levels_own, _, width = alpha.shape
    _, levels, own_rows, _ = ens_pert.shape
    chunks = own_rows // ROWS
    units = chunks * (members // PAIR)
    stacked = levels * ROWS
    levels_out = levels // n_mem
    factor = 1.0 / math.sqrt(members * n_mem)
    hbm = pl.BlockSpec(memory_space=pltpu.HBM)
    half, full = jnp.bfloat16, jnp.float32
    return pl.pallas_call(
        functools.partial(kernel, factor, n_lon, n_mem),
        out_shape=pltpu.VMEM((levels_out, own_rows, width), full),
        in_specs=[hbm] * 4,
        out_specs=pl.BlockSpec(memory_space=pltpu.VMEM),
        scratch_shapes=[
            pltpu.VMEM((chunks, members, levels, ROWS, width), half),
            pltpu.VMEM((chunks, members, levels, ROWS, width), half),
            pltpu.VMEM((PAIR, *alpha.shape[1:]), half),
            pltpu.VMEM((levels, levels), half),
            pltpu.VMEM((stacked, stacked), half),
            pltpu.VMEM((PAIR * width, PAIR * width), half),
            pltpu.VMEM((stacked, width), full),
            pltpu.VMEM((stacked, PAIR * width), full),
            pltpu.VMEM((stacked, PAIR * width), half),
            pltpu.VMEM((chunks, levels, ROWS, width), half),
            pltpu.VMEM((chunks, n_mem // 2, 2 * levels_out, ROWS, width), half),
            pltpu.VMEM((chunks, levels_out, ROWS, width), full),
            pltpu.VMEM((chunks, levels_out, ROWS, width), half),
            pltpu.VMEM((chunks, levels_out, ROWS, width), half),
            pltpu.VMEM((n_mem, levels_out, ROWS, width), half),
            pltpu.SemaphoreType.DMA,
            pltpu.SemaphoreType.DMA((1 + PAIR,)),
            pltpu.SemaphoreType.DMA((chunks,)),
            pltpu.SemaphoreType.DMA((chunks,)),
            pltpu.SemaphoreType.DMA,
            pltpu.SemaphoreType.DMA((units + 1,)),
            pltpu.SemaphoreType.REGULAR,
            pltpu.SemaphoreType.DMA,
            pltpu.SemaphoreType.DMA((chunks,)),
            pltpu.SemaphoreType.DMA,
            pltpu.SemaphoreType.DMA((chunks,)),
            pltpu.SemaphoreType.DMA,
            pltpu.SemaphoreType.DMA,
        ],
        compiler_params=pltpu.CompilerParams(
            collective_id=0, has_side_effects=True, flags=FLAGS, vmem_limit_bytes=LIMIT * 2**20
        ),
    )(*(pltpu.with_memory_space_constraint(x, pltpu.HBM) for x in (alpha, ens_pert, vert_sqrt, lat_sqrt)))


def solution(mesh):
    placed = (P("mem", "lon", None, None), P("mem", None, "lon", None), P(), P())
    return jax.shard_map(
        local, mesh=mesh, in_specs=placed, out_specs=P("mem", "lon", None), check_vma=False
    )
```
